128 devices in a mesh: grp: 4 (over y), dev: 32 (over z, x, core).
Axes of the slice: x: 4, y: 4, z: 4, core: 2. Of those that a mesh axis runs over, the one named last changes fastest.
Arguments:
- feeder_state: float32 [12288, 24, 256], P(('grp', 'dev')), may hold values from -6 to 6
- feeder_load: bfloat16 [12288, 24, 256], P(('grp', 'dev')), may hold values from -6 to 6
- feeder_inverse: bfloat16 [12288, 256, 256], P(('grp', 'dev')), as said below
- coupling: bfloat16 [12288, 256], P(('grp', 'dev')), may hold values from -0.375 to 0.375
- feeder_bus: int32 [12288], P(('grp', 'dev')), may hold values from 0 to 16383
- bus_coupling: bfloat16 [16384, 16384], P(('grp', 'dev')), may hold values from -0.09375 to 0.09375
- bus_diagonal: float32 [16384], P(('grp', 'dev')), may hold values from 1 to 3
- bus_load: float32 [24, 16384], P(None, ('grp', 'dev')), may hold values from -6 to 6
- bus_state: float32 [24, 16384], P(None, ('grp', 'dev')), may hold values from -6 to 6
- barrier: float32 [2], replicated, may hold values from 0.5 to 4
- step_length: float32 [2], replicated, may hold values from 0.4 to 1
Outputs:
- feeder_final: float32 [12288, 24, 256], P(('grp', 'dev'))
- bus_final: float32 [24, 16384], P(None, ('grp', 'dev'))
The draws below stay inside these ranges and needn't reach their ends.
Inputs may be any that keep to these rules, and one draw needn't show every extreme that they name: `feeder_inverse`: each block is symmetric with a positive diagonal and is positive definite.
All inputs are finite; a program needn't handle non-finite values.
Results may differ from the reference program's by a relative error of at most 0.0022.
Values may be sent and summed in bfloat16 or wider, within the bound.
A program may use at most 128 MiB of HBM per device.

```python
import math
import jax
import jax.numpy as jnp
from jax import lax

NODES = 256
HOURS = 24
ITERS = 2
FEED_DEV = 96
FEEDERS = 12288
BUSES = 16384


def draw_feeder_inverse(key, part):
    first_key, second_key = jax.random.split(key)
    noise = jax.random.normal(first_key, (FEEDERS, NODES, NODES), jnp.float32)
    noise = noise / jnp.sqrt(jnp.float32(NODES))
    symmetric = 0.5 * (noise + jnp.swapaxes(noise, 1, 2))
    pivots = jax.random.uniform(second_key, (FEEDERS, NODES), jnp.float32, 2.0, 4.0)
    return (symmetric + pivots[:, :, None] * jnp.eye(NODES, dtype=jnp.float32)).astype(jnp.bfloat16)


def place_ends(entries, key, least, top_value):
    index_at = [jax.random.randint(jax.random.fold_in(key, axis), (), 0, length) for axis, length in enumerate(entries.shape)]
    longest = entries.shape.index(max(entries.shape))
    beside = index_at[:longest] + [(index_at[longest] + 1) % entries.shape[longest]] + index_at[longest + 1:]
    return entries.at[tuple(index_at)].set(least).at[tuple(beside)].set(top_value)


def block_levels(key, extent, shards, least, top_value):
    level, own = 1.0, jax.random.fold_in(key, 6)
    for position, parts in shards:
        heights = jnp.exp(jax.random.uniform(jax.random.fold_in(own, position), (parts,), jnp.float32, least / len(shards), top_value / len(shards)))
        level = level * jnp.repeat(heights, extent[position] // parts).reshape([-1 if axis == position else 1 for axis in range(len(extent))])
    return level


def scatter_about(own_key, shape, scale, bound, pieces=(), kind=jnp.bfloat16):
    entries = scale * jax.random.normal(own_key, shape, jnp.float32)
    if pieces:
        entries = entries * block_levels(own_key, shape, pieces, -0.22, 0.18)
    return jnp.clip(entries, -bound, bound).astype(kind)


def setup_inputs(seed: int = 0) -> dict:
    seeds = jax.random.split(jax.random.key(seed), 12)
    return {
        "feeder_state": scatter_about(seeds[0], (FEEDERS, HOURS, NODES), 1.0, 6.0, ((0, 128),), jnp.float32),
        "feeder_load": scatter_about(seeds[1], (FEEDERS, HOURS, NODES), 1.0, 6.0, ((0, 128),)),
        "feeder_inverse": draw_feeder_inverse(jax.random.fold_in(seeds[11], 71), 0),
        "coupling": scatter_about(seeds[3], (FEEDERS, NODES), NODES ** -0.5, 0.375, ((0, 128),)),
        "feeder_bus": place_ends(jax.random.randint(seeds[4], (FEEDERS,), 0, BUSES), jax.random.fold_in(seeds[4], 1), 0, BUSES - 1).astype(jnp.int32),
        "bus_coupling": scatter_about(seeds[5], (BUSES, BUSES), (BUSES // 4) ** -0.5, 0.09375, ((0, 128),)),
        "bus_diagonal": jnp.clip(1.0 + 2.0 * jax.random.uniform(seeds[6], (BUSES,), jnp.float32) ** block_levels(seeds[6], (BUSES,), ((0, 128),), -0.2, 0.2), 1.0, 3.0),
        "bus_load": scatter_about(seeds[7], (HOURS, BUSES), 1.0, 6.0, ((1, 128),), jnp.float32),
        "bus_state": scatter_about(seeds[8], (HOURS, BUSES), 1.0, 6.0, ((1, 128),), jnp.float32),
        "barrier": jnp.clip(jnp.exp(jax.random.uniform(seeds[9], (ITERS,), jnp.float32, math.log(0.5), math.log(4.0))), 0.5, 4.0),
        "step_length": jnp.clip(jax.random.uniform(seeds[10], (ITERS,), jnp.float32, 0.4, 1.0), 0.4, 1.0),
    }


def feeder_products(blocks, vectors):
    count = vectors.shape[1]
    grouped = blocks.reshape(-1, FEED_DEV, NODES, NODES)
    columns = vectors.reshape(-1, FEED_DEV, count, NODES)

    def one_group(pair_block):
        return jnp.einsum("fij,fhj->fhi", pair_block[0].astype(jnp.float32), pair_block[1].astype(jnp.float32), precision=lax.Precision.HIGHEST)

    solved = lax.map(one_group, (grouped, columns))
    return solved.reshape(-1, count, NODES)


def reference(feeder_state, feeder_load, feeder_inverse, coupling, feeder_bus, bus_coupling, bus_diagonal, bus_load, bus_state, barrier, step_length):
    sensitivity = coupling.astype(jnp.float32)
    response = feeder_products(feeder_inverse, coupling[:, None, :])[:, 0, :]
    schur = jnp.sum(sensitivity * response, axis=-1)
    bus_schur = jax.ops.segment_sum(schur, feeder_bus, BUSES)
    feeder_now = feeder_state
    bus_now = bus_state
    for iteration in range(ITERS):
        weight_mu = barrier[iteration]
        residual = (feeder_load.astype(jnp.float32) + weight_mu * jax.nn.sigmoid(-feeder_now)).astype(jnp.bfloat16)
        solved = feeder_products(feeder_inverse, residual)
        boundary = jnp.sum(solved * sensitivity[:, None, :], axis=-1)
        bus_totals = jax.ops.segment_sum(boundary, feeder_bus, BUSES).T
        bus_right = bus_load + weight_mu * jax.nn.sigmoid(-bus_now) - bus_totals
        pivots = bus_diagonal + weight_mu + bus_schur
        first_sweep = (bus_right / pivots).astype(jnp.bfloat16)
        coupled = jnp.dot(first_sweep, bus_coupling.T, preferred_element_type=jnp.float32)
        second_sweep = (bus_right - coupled) / pivots
        bus_now = bus_now + step_length[iteration] * second_sweep
        at_feeder = second_sweep[:, feeder_bus].T
        feeder_now = feeder_now + step_length[iteration] * (solved - response[:, None, :] * at_feeder[:, :, None])
    return feeder_now, bus_now
```

```python
import functools

import jax
import jax.numpy as jnp
from jax import lax
from jax.experimental import pallas as pl
from jax.experimental.pallas import tpu as pltpu
from jax.sharding import PartitionSpec as P

MESH = pl.DeviceIdType.MESH
BOTH = ("grp", "dev")
LANES = 128
CHUNK = 8

OFFSETS = sorted(
    [(a, b, c) for a in range(4) for b in range(4) for c in range(4) if a or b or c],
    key=lambda t: -sum(min(v, 4 - v) for v in t),
)
GROUPS = (0, 1, 3, 2)


def place():
    y, d = lax.axis_index("grp"), lax.axis_index("dev")
    return y, d // 8, (d // 2) % 4, d % 2


def device(y, z, x, c):
    return (y, z * 8 + x * 2 + c)


def chip_of(y, z, x):
    return (y * 4 + z) * 4 + x


def plane_of(plane, count=16):
    return pl.ds(plane * 16, count)


def announce():
    y, z, x, c = place()
    bar = pltpu.get_barrier_semaphore()
    for dy, dz, dx in OFFSETS:
        to = device((y + dy) % 4, (z + dz) % 4, (x + dx) % 4, c)
        pl.semaphore_signal(bar, inc=1, device_id=to, device_id_type=MESH)
    pl.semaphore_signal(bar, inc=1, device_id=device(y, z, x, 1 - c), device_id_type=MESH)


def all_here():
    pl.semaphore_wait(pltpu.get_barrier_semaphore(), len(OFFSETS) + 1)


def send(buf, sems):
    sent, came, _, _ = sems
    y, z, x, c = place()
    for dy, dz, dx in OFFSETS:
        pltpu.make_async_remote_copy(
            src_ref=buf.at[c, chip_of(y, z, x)],
            dst_ref=buf.at[c, chip_of(y, z, x)],
            send_sem=sent,
            recv_sem=came.at[dy],
            device_id=device((y + dy) % 4, (z + dz) % 4, (x + dx) % 4, c),
            device_id_type=MESH,
        ).start()


def bytes_of(ref, sem):
    pltpu.make_async_copy(ref, ref, sem).wait()


def pass_on(buf, sems, dy):
    _, came, handed, _ = sems
    y, z, x, c = place()
    plane = (y + 4 - dy) % 4
    bytes_of(buf.at[c, plane_of(plane, 16 if dy else 15)], came.at[dy])
    pltpu.make_async_remote_copy(
        src_ref=buf.at[c, plane_of(plane)],
        dst_ref=buf.at[c, plane_of(plane)],
        send_sem=handed,
        recv_sem=sems[3].at[dy],
        device_id=device(y, z, x, 1 - c),
        device_id_type=MESH,
    ).start()


def partner_came(buf, sems, dy):
    y, z, x, c = place()
    plane = (y + 4 - dy) % 4
    bytes_of(buf.at[1 - c, plane_of(plane)], sems[3].at[dy])
    return plane


def drained(buf, sems):
    sent, _, handed, _ = sems
    c = place()[3]
    bytes_of(buf.at[c, 0 : len(OFFSETS)], sent)
    bytes_of(buf.at[c], handed)


def plane_rows(buf, plane, tail=None):
    blocks = []
    for k in range(16):
        for c in range(2):
            block = buf[c, plane * 16 + k]
            if tail is not None:
                block = jnp.concatenate([block, tail(c, plane * 16 + k)], axis=0)
            blocks.append(block)
    return jnp.concatenate(blocks, axis=1)


def gather_dot(buf, sems, weights, tail=None):
    total = None

    def product(dy):
        plane = partner_came(buf, sems, dy)
        columns = pl.ds(pl.multiple_of(plane * (32 * LANES), LANES), 32 * LANES)
        return lax.dot_general(
            plane_rows(buf, plane, tail),
            weights[:, columns],
            (((1,), (1,)), ((), ())),
            preferred_element_type=jnp.float32,
        )

    for k, dy in enumerate(GROUPS):
        pass_on(buf, sems, dy)
        if k:
            part = product(GROUPS[k - 1])
            total = part if total is None else total + part
    return total + product(GROUPS[-1])


def kernel(
    state_hbm,
    load_hbm,
    inverse_hbm,
    coupling_ref,
    bus_ref,
    network_hbm,
    diagonal_ref,
    bus_load_ref,
    bus_state_ref,
    barrier_ref,
    step_ref,
    y_hbm,
    response_ref,
    at_ref,
    bus_final_ref,
    inverse,
    state,
    load,
    solved,
    network,
    owned,
    chosen,
    sensitivity,
    blocks,
    schur_all,
    ids_all,
    load_sems,
    out_sem,
    sent,
    came,
    handed,
    partner,
):
    feeders = state.shape[0]
    chunks = feeders // CHUNK
    hours = state.shape[1]
    y, z, x, c = place()
    chip = chip_of(y, z, x)
    me = chip * 2 + c

    def chunk_copies(k):
        at = pl.ds(k * CHUNK, CHUNK)
        return [
            pltpu.make_async_copy(inverse_hbm.at[at], inverse.at[at], load_sems.at[0, k]),
            pltpu.make_async_copy(state_hbm.at[at], state.at[at], load_sems.at[1, k]),
            pltpu.make_async_copy(load_hbm.at[at], load.at[at], load_sems.at[2, k]),
        ]

    @pl.loop(0, chunks)
    def _(k):
        for copy in chunk_copies(k):
            copy.start()

    network_copy = pltpu.make_async_copy(network_hbm, network, load_sems.at[3, 0])
    network_copy.start()
    announce()

    def sems(p):
        return sent.at[p], came.at[p], handed.at[p], partner.at[p]

    sensitivity[...] = coupling_ref[...].astype(jnp.float32)
    lane = lax.broadcasted_iota(jnp.int32, (hours + 8, LANES), 1)

    mu = barrier_ref[0]

    def first_chunk(k, edge):
        for copy in chunk_copies(k):
            copy.wait()
        start = pl.multiple_of(k * CHUNK, CHUNK)
        rows = sensitivity[pl.ds(start, CHUNK), :]
        responses = []
        for j in range(CHUNK):
            f = start + j
            row = rows[j : j + 1, :]
            right = load[f].astype(jnp.float32) + mu * jax.nn.sigmoid(-state[f])
            right = jnp.concatenate([right, jnp.broadcast_to(row, (8, row.shape[1]))], axis=0)
            product = jnp.dot(
                right.astype(jnp.bfloat16), inverse[f], preferred_element_type=jnp.float32
            )
            solved[f] = product[:hours]
            responses.append(product[hours : hours + 1])
            scaled = product * row
            term = jnp.sum(scaled[:, :LANES] + scaled[:, LANES:], axis=1, keepdims=True)
            edge = jnp.where(lane == f, term, edge)
        response_ref[pl.ds(start, CHUNK), :] = jnp.concatenate(responses, axis=0)
        return edge

    edge = lax.fori_loop(0, chunks, first_chunk, jnp.zeros((hours + 8, LANES), jnp.float32))

    own = (c, chip)
    all_here()
    ids_all[own] = jnp.full((1, LANES), -1, jnp.int32)
    ids_all[c, chip, :, 0:feeders] = bus_ref[...]
    send(ids_all, sems(0))
    schur_all[own] = edge[hours : hours + 1]
    send(schur_all, sems(1))
    blocks[0, c, chip] = edge[:hours].astype(jnp.bfloat16)
    send(blocks.at[0], sems(2))

    for dy in GROUPS:
        pass_on(ids_all, sems(0), dy)
    for dy in GROUPS:
        partner_came(ids_all, sems(0), dy)
    my_bus = me * LANES + lax.broadcasted_iota(jnp.int32, (LANES, LANES), 0)

    @pl.loop(0, 64)
    def _(k):
        for core in range(2):
            ids = ids_all[core, k]
            columns = pl.ds(pl.multiple_of((k * 2 + core) * LANES, LANES), LANES)
            owned[:, columns] = jnp.where(my_bus == ids, 1.0, 0.0).astype(jnp.bfloat16)

    for dy in GROUPS:
        pass_on(schur_all, sems(1), dy)
    for dy in GROUPS:
        partner_came(schur_all, sems(1), dy)
    row8 = lax.broadcasted_iota(jnp.int32, (8, LANES), 0)

    def schur_rows(core, k):
        whole = jnp.broadcast_to(schur_all[core, k], (8, LANES))
        high = whole.astype(jnp.bfloat16).astype(jnp.float32)
        rows = jnp.where(row8 == 0, high, jnp.where(row8 == 1, whole - high, 0.0))
        return rows.astype(jnp.bfloat16)

    totals = gather_dot(blocks.at[0], sems(2), owned, schur_rows)
    bus_schur = totals[hours : hours + 1] + totals[hours + 1 : hours + 2]
    totals = totals[:hours]

    def bus_phase(totals, mu, step, bus_now, p):
        right = bus_load_ref[...] + mu * jax.nn.sigmoid(-bus_now) - totals
        pivots = diagonal_ref[...] + mu + bus_schur
        blocks[p, c, chip] = (right / pivots).astype(jnp.bfloat16)
        send(blocks.at[p], sems(p + 2))
        if p == 1:
            network_copy.wait()
        coupled = gather_dot(blocks.at[p], sems(p + 2), network)
        second = (right - coupled) / pivots
        blocks[p + 1, c, chip] = second.astype(jnp.bfloat16)
        send(blocks.at[p + 1], sems(p + 3))
        return bus_now + step * second

    bus_now = bus_phase(totals, mu, step_ref[0], bus_state_ref[...], 1)

    my_ids = jnp.broadcast_to(ids_all[own], (LANES, LANES)).T
    along = lax.broadcasted_iota(jnp.int32, (LANES, LANES), 1)

    @pl.loop(0, 128)
    def _(k):
        columns = pl.ds(pl.multiple_of(k * LANES, LANES), LANES)
        chosen[:, columns] = jnp.where(my_ids == along + k * LANES, 1.0, 0.0).astype(jnp.bfloat16)

    at = step_ref[0] * gather_dot(blocks.at[2], sems(4), chosen)

    mu = barrier_ref[1]
    step = step_ref[0]

    def second_chunk(k, edge):
        start = pl.multiple_of(k * CHUNK, CHUNK)
        rows = response_ref[pl.ds(start, CHUNK), :]
        here = pltpu.roll(at, lax.rem(LANES - start, LANES), 1)
        for j in range(CHUNK):
            f = start + j
            row = rows[j : j + 1, :]
            now = state[f] + (step * solved[f] - row * here[:, j : j + 1])
            state[f] = now
            residual = (load[f].astype(jnp.float32) + mu * jax.nn.sigmoid(-now)).astype(jnp.bfloat16)
            load[f] = residual
            scaled = residual.astype(jnp.float32) * row
            term = jnp.sum(scaled[:, :LANES] + scaled[:, LANES:], axis=1, keepdims=True)
            edge = jnp.where(lane[:hours] == f, term, edge)
        return edge

    edge = lax.fori_loop(0, chunks, second_chunk, jnp.zeros((hours, LANES), jnp.float32))
    blocks[3, c, chip] = edge.astype(jnp.bfloat16)
    send(blocks.at[3], sems(5))

    def y_copy(k):
        at = pl.ds(k * CHUNK, CHUNK)
        return pltpu.make_async_copy(solved.at[at], y_hbm.at[at], out_sem.at[k])

    last_step = step_ref[1]

    @pl.loop(0, chunks)
    def _(k):
        for j in range(CHUNK):
            f = k * CHUNK + j
            product = jnp.dot(load[f], inverse[f], preferred_element_type=jnp.float32)
            solved[f] = state[f] + last_step * product
        y_copy(k).start()

    totals = gather_dot(blocks.at[3], sems(5), owned)
    bus_final_ref[...] = bus_phase(totals, mu, last_step, bus_now, 4)
    at_ref[...] = last_step * gather_dot(blocks.at[5], sems(7), chosen)

    @pl.loop(0, chunks)
    def _(k):
        y_copy(k).wait()

    drained(ids_all, sems(0))
    drained(schur_all, sems(1))
    for p in range(6):
        drained(blocks.at[p], sems(p + 2))


def on_device(
    feeder_state,
    feeder_load,
    feeder_inverse,
    coupling,
    feeder_bus,
    bus_coupling,
    bus_diagonal,
    bus_load,
    bus_state,
    barrier,
    step_length,
):
    feeders, hours, nodes = feeder_state.shape
    owned, buses = bus_coupling.shape
    f32, bf16 = jnp.float32, jnp.bfloat16
    vmem, smem = pl.BlockSpec(memory_space=pltpu.VMEM), pl.BlockSpec(memory_space=pltpu.SMEM)
    hbm = pl.BlockSpec(memory_space=pl.ANY)
    chunks = feeders // CHUNK
    y, response, at, bus_final = pl.pallas_call(
        kernel,
        name="interior_point",
        out_shape=[
            jax.ShapeDtypeStruct((feeders, hours, nodes), f32),
            jax.ShapeDtypeStruct((feeders, nodes), f32),
            jax.ShapeDtypeStruct((hours, LANES), f32),
            jax.ShapeDtypeStruct((hours, owned), f32),
        ],
        in_specs=[hbm, hbm, hbm, vmem, vmem, hbm, vmem, vmem, vmem, smem, smem],
        out_specs=[hbm, vmem, vmem, vmem],
        scratch_shapes=[
            pltpu.VMEM((feeders, nodes, nodes), bf16),
            pltpu.VMEM((feeders, hours, nodes), f32),
            pltpu.VMEM((feeders, hours, nodes), bf16),
            pltpu.VMEM((feeders, hours, nodes), f32),
            pltpu.VMEM((owned, buses), bf16),
            pltpu.VMEM((LANES, 128 * LANES), bf16),
            pltpu.VMEM((LANES, buses), bf16),
            pltpu.VMEM((feeders, nodes), f32),
            pltpu.VMEM((6, 2, 64, hours, LANES), bf16),
            pltpu.VMEM((2, 64, 1, LANES), f32),
            pltpu.VMEM((2, 64, 1, LANES), jnp.int32),
            pltpu.SemaphoreType.DMA((4, chunks)),
            pltpu.SemaphoreType.DMA((chunks,)),
            pltpu.SemaphoreType.DMA((8,)),
            pltpu.SemaphoreType.DMA((8, 4)),
            pltpu.SemaphoreType.DMA((8,)),
            pltpu.SemaphoreType.DMA((8, 4)),
        ],
        compiler_params=pltpu.CompilerParams(
            collective_id=0, has_side_effects=True, vmem_limit_bytes=60 * 2**20
        ),
    )(
        feeder_state,
        feeder_load,
        feeder_inverse,
        coupling,
        feeder_bus.reshape(1, feeders),
        bus_coupling,
        bus_diagonal.reshape(1, owned),
        bus_load,
        bus_state,
        barrier,
        step_length,
    )
    at_feeder = at[:, :feeders].T
    return y - response[:, None, :] * at_feeder[:, :, None], bus_final


def solution(mesh):
    in_specs = (
        P(BOTH, None, None),
        P(BOTH, None, None),
        P(BOTH, None, None),
        P(BOTH, None),
        P(BOTH),
        P(BOTH, None),
        P(BOTH),
        P(None, BOTH),
        P(None, BOTH),
        P(),
        P(),
    )
    out_specs = (P(BOTH, None, None), P(None, BOTH))
    return jax.shard_map(
        on_device, mesh=mesh, in_specs=in_specs, out_specs=out_specs, check_vma=False
    )
```

```python
import functools

import jax
import jax.numpy as jnp
from jax import lax
from jax.experimental import pallas as pl
from jax.experimental.pallas import tpu as pltpu
from jax.sharding import PartitionSpec as P

MESH = pl.DeviceIdType.MESH
BOTH = ("grp", "dev")
LANES = 128
CHUNK = 8
AHEAD = 4

OFFSETS = sorted(
    [(a, b, c) for a in range(4) for b in range(4) for c in range(4) if a or b or c],
    key=lambda t: -sum(min(v, 4 - v) for v in t),
)
GROUPS = (0, 1, 3, 2)


def place():
    y, d = lax.axis_index("grp"), lax.axis_index("dev")
    return y, d // 8, (d // 2) % 4, d % 2


def device(y, z, x, c):
    return (y, z * 8 + x * 2 + c)


def chip_of(y, z, x):
    return (y * 4 + z) * 4 + x


def plane_of(plane, count=16):
    return pl.ds(plane * 16, count)


def announce():
    y, z, x, c = place()
    bar = pltpu.get_barrier_semaphore()
    for dy, dz, dx in OFFSETS:
        to = device((y + dy) % 4, (z + dz) % 4, (x + dx) % 4, c)
        pl.semaphore_signal(bar, inc=1, device_id=to, device_id_type=MESH)
    pl.semaphore_signal(bar, inc=1, device_id=device(y, z, x, 1 - c), device_id_type=MESH)


def all_here():
    pl.semaphore_wait(pltpu.get_barrier_semaphore(), len(OFFSETS) + 1)


def send(buf, sems):
    y, z, x, c = place()
    chip = chip_of(y, z, x)
    for dy, dz, dx in OFFSETS:
        pltpu.make_async_remote_copy(
            src_ref=buf.at[chip],
            dst_ref=buf.at[chip],
            send_sem=sems[0],
            recv_sem=sems[1].at[dy],
            device_id=device((y + dy) % 4, (z + dz) % 4, (x + dx) % 4, c),
            device_id_type=MESH,
        ).start()


def bytes_of(ref, sem):
    pltpu.make_async_copy(ref, ref, sem).wait()


def came(buf, sems, dy):
    plane = (place()[0] + 4 - dy) % 4
    bytes_of(buf.at[plane_of(plane, 16 if dy else 15)], sems[1].at[dy])
    return plane


def to_partner(src, dst, send_sem, recv_sem):
    y, z, x, c = place()
    return pltpu.make_async_remote_copy(
        src_ref=src,
        dst_ref=dst,
        send_sem=send_sem,
        recv_sem=recv_sem,
        device_id=device(y, z, x, 1 - c),
        device_id_type=MESH,
    )


def gather_dot(buf, sems, weights, theirs, ours):
    total = None
    for dy in GROUPS:
        plane = came(buf, sems, dy)
        columns = pl.ds(pl.multiple_of(plane * (16 * LANES), LANES), 16 * LANES)
        part = lax.dot_general(
            jnp.concatenate([buf[plane * 16 + k] for k in range(16)], axis=1),
            weights[:, columns],
            (((1,), (1,)), ((), ())),
            preferred_element_type=jnp.float32,
        )
        total = part if total is None else total + part
    rows = total.shape[0]
    theirs[0:rows] = total[:, LANES:]
    copy = to_partner(theirs.at[0:rows], ours.at[0:rows], sems[2], sems[3])
    copy.start()
    copy.wait()
    return total[:, :LANES] + ours[0:rows]


def kernel(
    state_hbm,
    load_hbm,
    inverse_hbm,
    coupling_ref,
    bus_ref,
    network_hbm,
    diagonal_ref,
    bus_load_ref,
    bus_state_ref,
    barrier_ref,
    step_ref,
    y_ref,
    response_ref,
    at_ref,
    bus_final_ref,
    inverse,
    state,
    load,
    solved,
    network,
    owned,
    chosen,
    sensitivity,
    blocks0,
    blocks,
    ids_all,
    my_ids,
    their_ids,
    theirs,
    ours,
    load_sems,
    net_sems,
    sent,
    arrived,
    half_sent,
    half_came,
):
    feeders = state.shape[0]
    chunks = feeders // CHUNK
    hours = state.shape[1]
    y, z, x, c = place()
    chip = chip_of(y, z, x)

    def chunk_copies(k):
        at = pl.ds(k * CHUNK, CHUNK)
        return [
            pltpu.make_async_copy(inverse_hbm.at[at], inverse.at[at], load_sems.at[0, k]),
            pltpu.make_async_copy(state_hbm.at[at], state.at[at], load_sems.at[1, k]),
            pltpu.make_async_copy(load_hbm.at[at], load.at[at], load_sems.at[2, k]),
        ]

    def start(k):
        for copy in chunk_copies(k):
            copy.start()

    for k in range(AHEAD):
        start(k)
    announce()

    def block_columns(k, core):
        return pl.ds(pl.multiple_of((k * 2 + core) * LANES, LANES), LANES)

    def columns_of(k):
        return pl.ds(pl.multiple_of(k * LANES, LANES), LANES)

    def sems(p):
        return sent.at[p], arrived.at[p], half_sent.at[p], half_came.at[p]

    sensitivity[...] = coupling_ref[...].astype(jnp.float32)
    lane = lax.broadcasted_iota(jnp.int32, (hours + 8, LANES), 1)

    mu = barrier_ref[0]

    def first_chunk(k, edge):
        for copy in chunk_copies(k):
            copy.wait()
        start = pl.multiple_of(k * CHUNK, CHUNK)
        rows = sensitivity[pl.ds(start, CHUNK), :]
        responses = []
        for j in range(CHUNK):
            f = start + j
            row = rows[j : j + 1, :]
            right = load[f].astype(jnp.float32) + mu * jax.nn.sigmoid(-state[f])
            right = jnp.concatenate([right, jnp.broadcast_to(row, (8, row.shape[1]))], axis=0)
            product = jnp.dot(
                right.astype(jnp.bfloat16), inverse[f], preferred_element_type=jnp.float32
            )
            solved[f] = product[:hours]
            responses.append(product[hours : hours + 1])
            scaled = product * row
            term = jnp.sum(scaled[:, :LANES] + scaled[:, LANES:], axis=1, keepdims=True)
            edge = jnp.where(lane == f, term, edge)
        response_ref[pl.ds(start, CHUNK), :] = jnp.concatenate(responses, axis=0)
        return edge

    def first_with_next(k, edge):
        start(k + AHEAD)
        return first_chunk(k, edge)

    edge = lax.fori_loop(
        0, chunks - AHEAD, first_with_next, jnp.zeros((hours + 8, LANES), jnp.float32)
    )

    all_here()
    my_ids[...] = jnp.full((1, LANES), -1, jnp.int32)
    my_ids[:, 0:feeders] = bus_ref[...]
    ids_all[chip] = my_ids[...]
    send(ids_all, sems(0))
    ids_copy = to_partner(my_ids, their_ids, half_sent.at[0], half_came.at[0])
    ids_copy.start()

    edge = lax.fori_loop(chunks - AHEAD, chunks, first_chunk, edge)
    row8 = lax.broadcasted_iota(jnp.int32, (8, LANES), 0)
    schur = edge[hours:]
    high = schur.astype(jnp.bfloat16).astype(jnp.float32)
    schur = jnp.where(row8 == 0, high, jnp.where(row8 == 1, schur - high, 0.0))
    blocks0[chip] = jnp.concatenate([edge[:hours], schur], axis=0).astype(jnp.bfloat16)
    send(blocks0, sems(1))

    @pl.loop(0, 64)
    def _(k):
        pltpu.make_async_copy(
            network_hbm.at[:, block_columns(k, c)],
            network.at[0:LANES, columns_of(k)],
            net_sems.at[0],
        ).start()
        to_partner(
            network_hbm.at[:, block_columns(k, 1 - c)],
            network.at[LANES : 2 * LANES, columns_of(k)],
            net_sems.at[1],
            net_sems.at[2],
        ).start()


    for dy in GROUPS:
        came(ids_all, sems(0), dy)
    ids_copy.wait()
    row256 = lax.broadcasted_iota(jnp.int32, (2 * LANES, LANES), 0)
    mine = row256 < LANES
    my_bus = jnp.where(
        mine, (chip * 2 + c) * LANES + row256, (chip * 2 + 1 - c) * LANES + row256 - LANES
    )

    @pl.loop(0, 64)
    def _(k):
        owned[:, columns_of(k)] = jnp.where(my_bus == ids_all[k], 1.0, 0.0).astype(jnp.bfloat16)

    hung = jnp.concatenate(
        [
            jnp.broadcast_to(my_ids[...], (LANES, LANES)).T,
            jnp.broadcast_to(their_ids[...], (LANES, LANES)).T,
        ],
        axis=0,
    )
    along = lax.broadcasted_iota(jnp.int32, (2 * LANES, LANES), 1)

    @pl.loop(0, 64)
    def _(k):
        buses = along + (k * 2 + c) * LANES
        chosen[:, columns_of(k)] = jnp.where(hung == buses, 1.0, 0.0).astype(jnp.bfloat16)

    totals = gather_dot(blocks0, sems(1), owned, theirs.at[0], ours.at[0])
    bus_schur = totals[hours : hours + 1] + totals[hours + 1 : hours + 2]
    totals = totals[:hours]

    def bus_phase(totals, mu, step, bus_now, p):
        right = bus_load_ref[...] + mu * jax.nn.sigmoid(-bus_now) - totals
        pivots = diagonal_ref[...] + mu + bus_schur
        blocks[p, chip] = (right / pivots).astype(jnp.bfloat16)
        send(blocks.at[p], sems(p + 2))
        if p == 0:
            bytes_of(network.at[0:LANES], net_sems.at[0])
            bytes_of(network.at[LANES : 2 * LANES], net_sems.at[2])
        coupled = gather_dot(
            blocks.at[p], sems(p + 2), network, theirs.at[p + 1], ours.at[p + 1]
        )
        second = (right - coupled) / pivots
        blocks[p + 1, chip] = second.astype(jnp.bfloat16)
        send(blocks.at[p + 1], sems(p + 3))
        return bus_now + step * second

    bus_now = bus_phase(totals, mu, step_ref[0], bus_state_ref[...], 0)

    at = step_ref[0] * gather_dot(blocks.at[1], sems(3), chosen, theirs.at[2], ours.at[2])

    mu = barrier_ref[1]
    step = step_ref[0]

    def second_chunk(k, edge):
        start = pl.multiple_of(k * CHUNK, CHUNK)
        rows = response_ref[pl.ds(start, CHUNK), :]
        here = pltpu.roll(at, lax.rem(LANES - start, LANES), 1)
        for j in range(CHUNK):
            f = start + j
            row = rows[j : j + 1, :]
            now = state[f] + (step * solved[f] - row * here[:, j : j + 1])
            state[f] = now
            residual = (load[f].astype(jnp.float32) + mu * jax.nn.sigmoid(-now)).astype(jnp.bfloat16)
            load[f] = residual
            scaled = residual.astype(jnp.float32) * row
            term = jnp.sum(scaled[:, :LANES] + scaled[:, LANES:], axis=1, keepdims=True)
            edge = jnp.where(lane[:hours] == f, term, edge)
        return edge

    edge = lax.fori_loop(0, chunks, second_chunk, jnp.zeros((hours, LANES), jnp.float32))
    blocks[2, chip] = edge.astype(jnp.bfloat16)
    send(blocks.at[2], sems(4))
    last_step = step_ref[1]

    @pl.loop(0, chunks)
    def _(k):
        for j in range(CHUNK):
            f = k * CHUNK + j
            product = jnp.dot(load[f], inverse[f], preferred_element_type=jnp.float32)
            y_ref[f] = state[f] + last_step * product

    totals = gather_dot(blocks.at[2], sems(4), owned, theirs.at[3], ours.at[3])
    bus_final_ref[...] = bus_phase(totals, mu, last_step, bus_now, 3)
    at_ref[...] = last_step * gather_dot(blocks.at[4], sems(6), chosen, theirs.at[5], ours.at[5])

    bytes_of(network.at[LANES : 2 * LANES], net_sems.at[1])
    others = pl.ds(0, len(OFFSETS))
    bytes_of(ids_all.at[others], sent.at[0])
    bytes_of(blocks0.at[others], sent.at[1])
    for p in range(5):
        bytes_of(blocks.at[p, others], sent.at[p + 2])


def last_kernel(y_ref, response_ref, at_ref, bus_ref, out_hbm, bus_final_ref, out, sem):
    feeders = y_ref.shape[0]
    bus_final_ref[...] = bus_ref[...]

    def copy(k):
        rows = pl.ds(k * CHUNK, CHUNK)
        return pltpu.make_async_copy(out.at[rows], out_hbm.at[rows], sem.at[k])

    for k in range(feeders // CHUNK):
        for f in range(k * CHUNK, (k + 1) * CHUNK):
            out[f] = y_ref[f] - response_ref[f : f + 1, :] * at_ref[:, f : f + 1]
        copy(k).start()
    for k in range(feeders // CHUNK):
        copy(k).wait()


def on_device(
    feeder_state,
    feeder_load,
    feeder_inverse,
    coupling,
    feeder_bus,
    bus_coupling,
    bus_diagonal,
    bus_load,
    bus_state,
    barrier,
    step_length,
):
    feeders, hours, nodes = feeder_state.shape
    owned, buses = bus_coupling.shape
    f32, bf16 = jnp.float32, jnp.bfloat16
    vmem, smem = pl.BlockSpec(memory_space=pltpu.VMEM), pl.BlockSpec(memory_space=pltpu.SMEM)
    hbm = pl.BlockSpec(memory_space=pltpu.HBM)
    chunks = feeders // CHUNK
    y, response, at, bus_last = pl.pallas_call(
        kernel,
        name="interior_point",
        out_shape=[
            pltpu.VMEM((feeders, hours, nodes), f32),
            pltpu.VMEM((feeders, nodes), f32),
            pltpu.VMEM((hours, LANES), f32),
            pltpu.VMEM((hours, owned), f32),
        ],
        in_specs=[hbm, hbm, hbm, vmem, vmem, hbm, vmem, vmem, vmem, smem, smem],
        out_specs=[vmem, vmem, vmem, vmem],
        scratch_shapes=[
            pltpu.VMEM((feeders, nodes, nodes), bf16),
            pltpu.VMEM((feeders, hours, nodes), f32),
            pltpu.VMEM((feeders, hours, nodes), bf16),
            pltpu.VMEM((feeders, hours, nodes), f32),
            pltpu.VMEM((2 * owned, buses // 2), bf16),
            pltpu.VMEM((2 * owned, 64 * LANES), bf16),
            pltpu.VMEM((2 * LANES, buses // 2), bf16),
            pltpu.VMEM((feeders, nodes), f32),
            pltpu.VMEM((64, hours + 8, LANES), bf16),
            pltpu.VMEM((5, 64, hours, LANES), bf16),
            pltpu.VMEM((64, 1, LANES), jnp.int32),
            pltpu.VMEM((1, LANES), jnp.int32),
            pltpu.VMEM((1, LANES), jnp.int32),
            pltpu.VMEM((6, hours + 8, LANES), f32),
            pltpu.VMEM((6, hours + 8, LANES), f32),
            pltpu.SemaphoreType.DMA((3, chunks)),
            pltpu.SemaphoreType.DMA((3,)),
            pltpu.SemaphoreType.DMA((7,)),
            pltpu.SemaphoreType.DMA((7, 4)),
            pltpu.SemaphoreType.DMA((7,)),
            pltpu.SemaphoreType.DMA((7,)),
        ],
        compiler_params=pltpu.CompilerParams(
            collective_id=0, has_side_effects=True, vmem_limit_bytes=64_430_080
        ),
    )(
        feeder_state,
        feeder_load,
        feeder_inverse,
        coupling,
        feeder_bus.reshape(1, feeders),
        bus_coupling,
        bus_diagonal.reshape(1, owned),
        bus_load,
        bus_state,
        barrier,
        step_length,
    )
    return pl.pallas_call(
        last_kernel,
        name="last_update",
        out_shape=[
            jax.ShapeDtypeStruct((feeders, hours, nodes), f32),
            jax.ShapeDtypeStruct((hours, owned), f32),
        ],
        in_specs=[vmem, vmem, vmem, vmem],
        out_specs=[hbm, vmem],
        scratch_shapes=[
            pltpu.VMEM((feeders, hours, nodes), f32),
            pltpu.SemaphoreType.DMA((chunks,)),
        ],
        compiler_params=pltpu.CompilerParams(vmem_limit_bytes=8 * 2**20),
    )(y, response, at, bus_last)


def solution(mesh):
    in_specs = (
        P(BOTH, None, None),
        P(BOTH, None, None),
        P(BOTH, None, None),
        P(BOTH, None),
        P(BOTH),
        P(BOTH, None),
        P(BOTH),
        P(None, BOTH),
        P(None, BOTH),
        P(),
        P(),
    )
    out_specs = (P(BOTH, None, None), P(None, BOTH))
    return jax.shard_map(
        on_device, mesh=mesh, in_specs=in_specs, out_specs=out_specs, check_vma=False
    )
```

```python
import functools

import jax
import jax.numpy as jnp
from jax import lax
from jax.experimental import pallas as pl
from jax.experimental.pallas import tpu as pltpu
from jax.sharding import PartitionSpec as P

MESH = pl.DeviceIdType.MESH
BOTH = ("grp", "dev")
LANES = 128
CHUNK = 8
AHEAD = 4

OFFSETS = sorted(
    [(a, b, c) for a in range(4) for b in range(4) for c in range(4) if a or b or c],
    key=lambda t: -sum(min(v, 4 - v) for v in t),
)
GROUPS = (0, 1, 3, 2)


def place():
    y, d = lax.axis_index("grp"), lax.axis_index("dev")
    return y, d // 8, (d // 2) % 4, d % 2


def device(y, z, x, c):
    return (y, z * 8 + x * 2 + c)


def chip_of(y, z, x):
    return (y * 4 + z) * 4 + x


def plane_of(plane, count=16):
    return pl.ds(plane * 16, count)


def announce():
    y, z, x, c = place()
    bar = pltpu.get_barrier_semaphore()
    for dy, dz, dx in OFFSETS:
        to = device((y + dy) % 4, (z + dz) % 4, (x + dx) % 4, c)
        pl.semaphore_signal(bar, inc=1, device_id=to, device_id_type=MESH)
    pl.semaphore_signal(bar, inc=1, device_id=device(y, z, x, 1 - c), device_id_type=MESH)


def all_here():
    pl.semaphore_wait(pltpu.get_barrier_semaphore(), len(OFFSETS) + 1)


def send(buf, sems):
    y, z, x, c = place()
    chip = chip_of(y, z, x)
    for dy, dz, dx in OFFSETS:
        pltpu.make_async_remote_copy(
            src_ref=buf.at[chip],
            dst_ref=buf.at[chip],
            send_sem=sems[0],
            recv_sem=sems[1].at[dy],
            device_id=device((y + dy) % 4, (z + dz) % 4, (x + dx) % 4, c),
            device_id_type=MESH,
        ).start()


def bytes_of(ref, sem):
    pltpu.make_async_copy(ref, ref, sem).wait()


def came(buf, sems, dy):
    plane = (place()[0] + 4 - dy) % 4
    bytes_of(buf.at[plane_of(plane, 16 if dy else 15)], sems[1].at[dy])
    return plane


def to_partner(src, dst, send_sem, recv_sem):
    y, z, x, c = place()
    return pltpu.make_async_remote_copy(
        src_ref=src,
        dst_ref=dst,
        send_sem=send_sem,
        recv_sem=recv_sem,
        device_id=device(y, z, x, 1 - c),
        device_id_type=MESH,
    )


def gather_dot(buf, sems, weights, theirs, ours, turned=False):
    total = None
    for dy in GROUPS:
        plane = came(buf, sems, dy)
        columns = pl.ds(pl.multiple_of(plane * (16 * LANES), LANES), 16 * LANES)
        here = jnp.concatenate([buf[plane * 16 + k] for k in range(16)], axis=1)
        if turned:
            part = jnp.dot(here, weights[columns, :], preferred_element_type=jnp.float32)
        else:
            part = lax.dot_general(
                weights[:, columns],
                here,
                (((1,), (1,)), ((), ())),
                preferred_element_type=jnp.float32,
            )
        total = part if total is None else total + part
    rows = buf.shape[1]
    if not turned:
        empty = jnp.zeros((total.shape[0], LANES - rows), jnp.float32)
        total = jnp.concatenate([total, empty], axis=1).T[:rows]
    theirs[0:rows] = total[:, LANES:]
    copy = to_partner(theirs.at[0:rows], ours.at[0:rows], sems[2], sems[3])
    copy.start()
    copy.wait()
    return total[:, :LANES] + ours[0:rows]


def kernel(
    state_hbm,
    load_hbm,
    inverse_hbm,
    coupling_ref,
    bus_ref,
    network_hbm,
    diagonal_ref,
    bus_load_ref,
    bus_state_ref,
    barrier_ref,
    step_ref,
    y_ref,
    response_ref,
    at_ref,
    bus_final_ref,
    inverse,
    state,
    load,
    solved,
    network,
    owned,
    chosen,
    sensitivity,
    blocks0,
    blocks,
    ids_all,
    my_ids,
    their_ids,
    theirs,
    ours,
    owned_turned,
    network_turned,
    load_sems,
    net_sems,
    sent,
    arrived,
    half_sent,
    half_came,
):
    feeders = state.shape[0]
    chunks = feeders // CHUNK
    hours = state.shape[1]
    y, z, x, c = place()
    chip = chip_of(y, z, x)

    def chunk_copies(k):
        at = pl.ds(k * CHUNK, CHUNK)
        return [
            pltpu.make_async_copy(inverse_hbm.at[at], inverse.at[at], load_sems.at[0, k]),
            pltpu.make_async_copy(state_hbm.at[at], state.at[at], load_sems.at[1, k]),
            pltpu.make_async_copy(load_hbm.at[at], load.at[at], load_sems.at[2, k]),
        ]

    def start(k):
        for copy in chunk_copies(k):
            copy.start()

    for k in range(AHEAD):
        start(k)
    announce()

    def block_columns(k, core):
        return pl.ds(pl.multiple_of((k * 2 + core) * LANES, LANES), LANES)

    def columns_of(k):
        return pl.ds(pl.multiple_of(k * LANES, LANES), LANES)

    def sems(p):
        return sent.at[p], arrived.at[p], half_sent.at[p], half_came.at[p]

    sensitivity[...] = coupling_ref[...].astype(jnp.float32)
    lane = lax.broadcasted_iota(jnp.int32, (hours + 8, LANES), 1)

    mu = barrier_ref[0]

    def first_chunk(k, edge):
        for copy in chunk_copies(k):
            copy.wait()
        start = pl.multiple_of(k * CHUNK, CHUNK)
        rows = sensitivity[pl.ds(start, CHUNK), :]
        responses = []
        for j in range(CHUNK):
            f = start + j
            row = rows[j : j + 1, :]
            right = load[f].astype(jnp.float32) + mu * jax.nn.sigmoid(-state[f])
            right = jnp.concatenate([right, jnp.broadcast_to(row, (8, row.shape[1]))], axis=0)
            product = jnp.dot(
                right.astype(jnp.bfloat16), inverse[f], preferred_element_type=jnp.float32
            )
            solved[f] = product[:hours]
            responses.append(product[hours : hours + 1])
            scaled = product * row
            term = jnp.sum(scaled[:, :LANES] + scaled[:, LANES:], axis=1, keepdims=True)
            edge = jnp.where(lane == f, term, edge)
        response_ref[pl.ds(start, CHUNK), :] = jnp.concatenate(responses, axis=0)
        return edge

    def first_with_next(k, edge):
        start(k + AHEAD)
        return first_chunk(k, edge)

    edge = lax.fori_loop(
        0, chunks - AHEAD, first_with_next, jnp.zeros((hours + 8, LANES), jnp.float32)
    )

    all_here()
    my_ids[...] = jnp.full((1, LANES), -1, jnp.int32)
    my_ids[:, 0:feeders] = bus_ref[...]
    ids_all[chip] = my_ids[...]
    send(ids_all, sems(0))
    ids_copy = to_partner(my_ids, their_ids, half_sent.at[0], half_came.at[0])
    ids_copy.start()

    edge = lax.fori_loop(chunks - AHEAD, chunks, first_chunk, edge)
    row8 = lax.broadcasted_iota(jnp.int32, (8, LANES), 0)
    schur = edge[hours:]
    high = schur.astype(jnp.bfloat16).astype(jnp.float32)
    schur = jnp.where(row8 == 0, high, jnp.where(row8 == 1, schur - high, 0.0))
    blocks0[chip] = jnp.concatenate([edge[:hours], schur], axis=0).astype(jnp.bfloat16)
    send(blocks0, sems(1))

    @pl.loop(0, 64)
    def _(k):
        pltpu.make_async_copy(
            network_hbm.at[:, block_columns(k, c)],
            network.at[0:LANES, columns_of(k)],
            net_sems.at[0],
        ).start()
        to_partner(
            network_hbm.at[:, block_columns(k, 1 - c)],
            network.at[LANES : 2 * LANES, columns_of(k)],
            net_sems.at[1],
            net_sems.at[2],
        ).start()


    for dy in GROUPS:
        came(ids_all, sems(0), dy)
    ids_copy.wait()
    row256 = lax.broadcasted_iota(jnp.int32, (2 * LANES, LANES), 0)
    mine = row256 < LANES
    my_bus = jnp.where(
        mine, (chip * 2 + c) * LANES + row256, (chip * 2 + 1 - c) * LANES + row256 - LANES
    )

    @pl.loop(0, 64)
    def _(k):
        owned[:, columns_of(k)] = jnp.where(my_bus == ids_all[k], 1.0, 0.0).astype(jnp.bfloat16)

    hung = jnp.concatenate([my_ids[...], their_ids[...]], axis=1)
    down = lax.broadcasted_iota(jnp.int32, (LANES, 2 * LANES), 0)

    @pl.loop(0, 64)
    def _(k):
        buses = down + (k * 2 + c) * LANES
        chosen[columns_of(k), :] = jnp.where(hung == buses, 1.0, 0.0).astype(jnp.bfloat16)

    totals = gather_dot(blocks0, sems(1), owned, theirs.at[0], ours.at[0])
    bus_schur = totals[hours : hours + 1] + totals[hours + 1 : hours + 2]
    totals = totals[:hours]

    def flip(src, dst):
        @pl.loop(0, 64)
        def _(k):
            dst[columns_of(k), :] = src[:, columns_of(k)].T

    def bus_phase(totals, mu, step, bus_now, p):
        right = bus_load_ref[...] + mu * jax.nn.sigmoid(-bus_now) - totals
        pivots = diagonal_ref[...] + mu + bus_schur
        blocks[p, chip] = (right / pivots).astype(jnp.bfloat16)
        send(blocks.at[p], sems(p + 2))
        if p == 0:
            bytes_of(network.at[0:LANES], net_sems.at[0])
            bytes_of(network.at[LANES : 2 * LANES], net_sems.at[2])
            flip(owned, owned_turned)
        coupled = gather_dot(
            blocks.at[p],
            sems(p + 2),
            network_turned if p else network,
            theirs.at[p + 1],
            ours.at[p + 1],
            p > 0,
        )
        second = (right - coupled) / pivots
        blocks[p + 1, chip] = second.astype(jnp.bfloat16)
        send(blocks.at[p + 1], sems(p + 3))
        return bus_now + step * second

    bus_now = bus_phase(totals, mu, step_ref[0], bus_state_ref[...], 0)

    flip(network, network_turned)
    at = step_ref[0] * gather_dot(blocks.at[1], sems(3), chosen, theirs.at[2], ours.at[2], True)

    mu = barrier_ref[1]
    step = step_ref[0]

    def second_chunk(k, edge):
        start = pl.multiple_of(k * CHUNK, CHUNK)
        rows = response_ref[pl.ds(start, CHUNK), :]
        here = pltpu.roll(at, lax.rem(LANES - start, LANES), 1)
        for j in range(CHUNK):
            f = start + j
            row = rows[j : j + 1, :]
            now = state[f] + (step * solved[f] - row * here[:, j : j + 1])
            state[f] = now
            residual = (load[f].astype(jnp.float32) + mu * jax.nn.sigmoid(-now)).astype(jnp.bfloat16)
            load[f] = residual
            scaled = residual.astype(jnp.float32) * row
            term = jnp.sum(scaled[:, :LANES] + scaled[:, LANES:], axis=1, keepdims=True)
            edge = jnp.where(lane[:hours] == f, term, edge)
        return edge

    edge = lax.fori_loop(0, chunks, second_chunk, jnp.zeros((hours, LANES), jnp.float32))
    blocks[2, chip] = edge.astype(jnp.bfloat16)
    send(blocks.at[2], sems(4))
    last_step = step_ref[1]

    @pl.loop(0, chunks)
    def _(k):
        for j in range(CHUNK):
            f = k * CHUNK + j
            product = jnp.dot(load[f], inverse[f], preferred_element_type=jnp.float32)
            y_ref[f] = state[f] + last_step * product

    totals = gather_dot(blocks.at[2], sems(4), owned_turned, theirs.at[3], ours.at[3], True)
    bus_final_ref[...] = bus_phase(totals, mu, last_step, bus_now, 3)
    at_ref[...] = last_step * gather_dot(blocks.at[4], sems(6), chosen, theirs.at[5], ours.at[5], True)

    bytes_of(network.at[LANES : 2 * LANES], net_sems.at[1])
    others = pl.ds(0, len(OFFSETS))
    bytes_of(ids_all.at[others], sent.at[0])
    bytes_of(blocks0.at[others], sent.at[1])
    for p in range(5):
        bytes_of(blocks.at[p, others], sent.at[p + 2])


def last_kernel(y_ref, response_ref, at_ref, bus_ref, out_hbm, bus_final_ref, out, sem):
    feeders = y_ref.shape[0]
    bus_final_ref[...] = bus_ref[...]

    def copy(k):
        rows = pl.ds(k * CHUNK, CHUNK)
        return pltpu.make_async_copy(out.at[rows], out_hbm.at[rows], sem.at[k])

    for k in range(feeders // CHUNK):
        for f in range(k * CHUNK, (k + 1) * CHUNK):
            out[f] = y_ref[f] - response_ref[f : f + 1, :] * at_ref[:, f : f + 1]
        copy(k).start()
    for k in range(feeders // CHUNK):
        copy(k).wait()


def on_device(
    feeder_state,
    feeder_load,
    feeder_inverse,
    coupling,
    feeder_bus,
    bus_coupling,
    bus_diagonal,
    bus_load,
    bus_state,
    barrier,
    step_length,
):
    feeders, hours, nodes = feeder_state.shape
    owned, buses = bus_coupling.shape
    f32, bf16 = jnp.float32, jnp.bfloat16
    vmem, smem = pl.BlockSpec(memory_space=pltpu.VMEM), pl.BlockSpec(memory_space=pltpu.SMEM)
    hbm = pl.BlockSpec(memory_space=pltpu.HBM)
    chunks = feeders // CHUNK
    y, response, at, bus_last = pl.pallas_call(
        kernel,
        name="interior_point",
        out_shape=[
            pltpu.VMEM((feeders, hours, nodes), f32),
            pltpu.VMEM((feeders, nodes), f32),
            pltpu.VMEM((hours, LANES), f32),
            pltpu.VMEM((hours, owned), f32),
        ],
        in_specs=[hbm, hbm, hbm, vmem, vmem, hbm, vmem, vmem, vmem, smem, smem],
        out_specs=[vmem, vmem, vmem, vmem],
        scratch_shapes=[
            pltpu.VMEM((feeders, nodes, nodes), bf16),
            pltpu.VMEM((feeders, hours, nodes), f32),
            pltpu.VMEM((feeders, hours, nodes), bf16),
            pltpu.VMEM((feeders, hours, nodes), f32),
            pltpu.VMEM((2 * owned, buses // 2), bf16),
            pltpu.VMEM((2 * owned, 64 * LANES), bf16),
            pltpu.VMEM((buses // 2, 2 * LANES), bf16),
            pltpu.VMEM((feeders, nodes), f32),
            pltpu.VMEM((64, hours + 8, LANES), bf16),
            pltpu.VMEM((5, 64, hours, LANES), bf16),
            pltpu.VMEM((64, 1, LANES), jnp.int32),
            pltpu.VMEM((1, LANES), jnp.int32),
            pltpu.VMEM((1, LANES), jnp.int32),
            pltpu.VMEM((6, hours + 8, LANES), f32),
            pltpu.VMEM((6, hours + 8, LANES), f32),
            pltpu.VMEM((64 * LANES, 2 * owned), bf16),
            pltpu.VMEM((buses // 2, 2 * owned), bf16),
            pltpu.SemaphoreType.DMA((3, chunks)),
            pltpu.SemaphoreType.DMA((3,)),
            pltpu.SemaphoreType.DMA((7,)),
            pltpu.SemaphoreType.DMA((7, 4)),
            pltpu.SemaphoreType.DMA((7,)),
            pltpu.SemaphoreType.DMA((7,)),
        ],
        compiler_params=pltpu.CompilerParams(
            collective_id=0, has_side_effects=True, vmem_limit_bytes=64_430_080
        ),
    )(
        feeder_state,
        feeder_load,
        feeder_inverse,
        coupling,
        feeder_bus.reshape(1, feeders),
        bus_coupling,
        bus_diagonal.reshape(1, owned),
        bus_load,
        bus_state,
        barrier,
        step_length,
    )
    return pl.pallas_call(
        last_kernel,
        name="last_update",
        out_shape=[
            jax.ShapeDtypeStruct((feeders, hours, nodes), f32),
            jax.ShapeDtypeStruct((hours, owned), f32),
        ],
        in_specs=[vmem, vmem, vmem, vmem],
        out_specs=[hbm, vmem],
        scratch_shapes=[
            pltpu.VMEM((feeders, hours, nodes), f32),
            pltpu.SemaphoreType.DMA((chunks,)),
        ],
        compiler_params=pltpu.CompilerParams(vmem_limit_bytes=8 * 2**20),
    )(y, response, at, bus_last)


def solution(mesh):
    in_specs = (
        P(BOTH, None, None),
        P(BOTH, None, None),
        P(BOTH, None, None),
        P(BOTH, None),
        P(BOTH),
        P(BOTH, None),
        P(BOTH),
        P(None, BOTH),
        P(None, BOTH),
        P(),
        P(),
    )
    out_specs = (P(BOTH, None, None), P(None, BOTH))
    return jax.shard_map(
        on_device, mesh=mesh, in_specs=in_specs, out_specs=out_specs, check_vma=False
    )
```

```python
import functools

import jax
import jax.numpy as jnp
from jax import lax
from jax.experimental import pallas as pl
from jax.experimental.pallas import tpu as pltpu
from jax.sharding import PartitionSpec as P

MESH = pl.DeviceIdType.MESH
BOTH = ("grp", "dev")
LANES = 128
CHUNK = 8
AHEAD = 4

OFFSETS = sorted(
    [(a, b, c) for a in range(4) for b in range(4) for c in range(4) if a or b or c],
    key=lambda t: -sum(min(v, 4 - v) for v in t),
)
GROUPS = (0, 1, 3, 2)


def place():
    y, d = lax.axis_index("grp"), lax.axis_index("dev")
    return y, d // 8, (d // 2) % 4, d % 2


def device(y, z, x, c):
    return (y, z * 8 + x * 2 + c)


def chip_of(y, z, x):
    return (y * 4 + z) * 4 + x


def plane_of(plane, count=16):
    return pl.ds(plane * 16, count)


def announce():
    y, z, x, c = place()
    bar = pltpu.get_barrier_semaphore()
    for dy, dz, dx in OFFSETS:
        to = device((y + dy) % 4, (z + dz) % 4, (x + dx) % 4, c)
        pl.semaphore_signal(bar, inc=1, device_id=to, device_id_type=MESH)
    pl.semaphore_signal(bar, inc=1, device_id=device(y, z, x, 1 - c), device_id_type=MESH)


def all_here():
    pl.semaphore_wait(pltpu.get_barrier_semaphore(), len(OFFSETS) + 1)


def send(buf, sems):
    y, z, x, c = place()
    chip = chip_of(y, z, x)
    for dy, dz, dx in OFFSETS:
        pltpu.make_async_remote_copy(
            src_ref=buf.at[chip],
            dst_ref=buf.at[chip],
            send_sem=sems[0],
            recv_sem=sems[1].at[dy],
            device_id=device((y + dy) % 4, (z + dz) % 4, (x + dx) % 4, c),
            device_id_type=MESH,
        ).start()


def bytes_of(ref, sem):
    pltpu.make_async_copy(ref, ref, sem).wait()


def came(buf, sems, dy):
    plane = (place()[0] + 4 - dy) % 4
    bytes_of(buf.at[plane_of(plane, 16 if dy else 15)], sems[1].at[dy])
    return plane


def to_partner(src, dst, send_sem, recv_sem):
    y, z, x, c = place()
    return pltpu.make_async_remote_copy(
        src_ref=src,
        dst_ref=dst,
        send_sem=send_sem,
        recv_sem=recv_sem,
        device_id=device(y, z, x, 1 - c),
        device_id_type=MESH,
    )


def gather_dot(buf, sems, weights, theirs, ours, turned=False):
    total = None
    for dy in GROUPS:
        came(buf, sems, dy)
    for plane in range(4):
        columns = slice(plane * 16 * LANES, (plane + 1) * 16 * LANES)
        here = jnp.concatenate([buf[plane * 16 + k] for k in range(16)], axis=1)
        if turned:
            part = jnp.dot(here, weights[columns, :], preferred_element_type=jnp.float32)
        else:
            part = lax.dot_general(
                weights[:, columns],
                here,
                (((1,), (1,)), ((), ())),
                preferred_element_type=jnp.float32,
            )
        total = part if total is None else total + part
    rows = buf.shape[1]
    if not turned:
        empty = jnp.zeros((total.shape[0], LANES - rows), jnp.float32)
        total = jnp.concatenate([total, empty], axis=1).T[:rows]
    theirs[0:rows] = total[:, LANES:]
    copy = to_partner(theirs.at[0:rows], ours.at[0:rows], sems[2], sems[3])
    copy.start()
    copy.wait_recv()
    return total[:, :LANES] + ours[0:rows]


def kernel(
    state_hbm,
    load_hbm,
    inverse_hbm,
    coupling_ref,
    bus_ref,
    network_hbm,
    diagonal_ref,
    bus_load_ref,
    bus_state_ref,
    barrier_ref,
    step_ref,
    y_ref,
    response_ref,
    at_ref,
    bus_final_ref,
    inverse,
    state,
    load,
    solved,
    network,
    owned,
    chosen,
    sensitivity,
    blocks0,
    blocks,
    ids_all,
    my_ids,
    their_ids,
    theirs,
    ours,
    owned_turned,
    network_turned,
    load_sems,
    net_sems,
    sent,
    arrived,
    half_sent,
    half_came,
):
    feeders = state.shape[0]
    chunks = feeders // CHUNK
    hours = state.shape[1]
    y, z, x, c = place()
    chip = chip_of(y, z, x)

    def chunk_copies(k):
        at = pl.ds(k * CHUNK, CHUNK)
        return [
            pltpu.make_async_copy(inverse_hbm.at[at], inverse.at[at], load_sems.at[0, k]),
            pltpu.make_async_copy(state_hbm.at[at], state.at[at], load_sems.at[1, k]),
            pltpu.make_async_copy(load_hbm.at[at], load.at[at], load_sems.at[2, k]),
        ]

    def start(k):
        for copy in chunk_copies(k):
            copy.start()

    for k in range(AHEAD):
        start(k)
    announce()

    def block_columns(k, core):
        return pl.ds(pl.multiple_of((k * 2 + core) * LANES, LANES), LANES)

    def columns_of(k):
        return pl.ds(pl.multiple_of(k * LANES, LANES), LANES)

    def sems(p):
        return sent.at[p], arrived.at[p], half_sent.at[p], half_came.at[p]

    sensitivity[...] = coupling_ref[...].astype(jnp.float32)
    lane = lax.broadcasted_iota(jnp.int32, (hours + 8, LANES), 1)

    mu = barrier_ref[0]

    def first_chunk(k, edge):
        for copy in chunk_copies(k):
            copy.wait()
        start = pl.multiple_of(k * CHUNK, CHUNK)
        rows = sensitivity[pl.ds(start, CHUNK), :]
        responses = []
        for j in range(CHUNK):
            f = start + j
            row = rows[j : j + 1, :]
            right = load[f].astype(jnp.float32) + mu * jax.nn.sigmoid(-state[f])
            right = jnp.concatenate([right, jnp.broadcast_to(row, (8, row.shape[1]))], axis=0)
            product = jnp.dot(
                right.astype(jnp.bfloat16), inverse[f], preferred_element_type=jnp.float32
            )
            solved[f] = product[:hours]
            responses.append(product[hours : hours + 1])
            scaled = product * row
            term = jnp.sum(scaled[:, :LANES] + scaled[:, LANES:], axis=1, keepdims=True)
            edge = jnp.where(lane == f, term, edge)
        response_ref[pl.ds(start, CHUNK), :] = jnp.concatenate(responses, axis=0)
        return edge

    def first_with_next(k, edge):
        start(k + AHEAD)
        return first_chunk(k, edge)

    edge = lax.fori_loop(
        0, chunks - AHEAD, first_with_next, jnp.zeros((hours + 8, LANES), jnp.float32)
    )

    all_here()
    my_ids[...] = jnp.full((1, LANES), -1, jnp.int32)
    my_ids[:, 0:feeders] = bus_ref[...]
    ids_all[chip] = my_ids[...]
    send(ids_all, sems(0))
    ids_copy = to_partner(my_ids, their_ids, half_sent.at[0], half_came.at[0])
    ids_copy.start()

    edge = lax.fori_loop(chunks - AHEAD, chunks, first_chunk, edge)
    row8 = lax.broadcasted_iota(jnp.int32, (8, LANES), 0)
    schur = edge[hours:]
    high = schur.astype(jnp.bfloat16).astype(jnp.float32)
    schur = jnp.where(row8 == 0, high, jnp.where(row8 == 1, schur - high, 0.0))
    blocks0[chip] = jnp.concatenate([edge[:hours], schur], axis=0).astype(jnp.bfloat16)
    send(blocks0, sems(1))

    @pl.loop(0, 64)
    def _(k):
        pltpu.make_async_copy(
            network_hbm.at[:, block_columns(k, c)],
            network.at[0:LANES, columns_of(k)],
            net_sems.at[0],
        ).start()
        to_partner(
            network_hbm.at[:, block_columns(k, 1 - c)],
            network.at[LANES : 2 * LANES, columns_of(k)],
            net_sems.at[1],
            net_sems.at[2],
        ).start()


    for dy in GROUPS:
        came(ids_all, sems(0), dy)
    ids_copy.wait()
    row256 = lax.broadcasted_iota(jnp.int32, (2 * LANES, LANES), 0)
    mine = row256 < LANES
    my_bus = jnp.where(
        mine, (chip * 2 + c) * LANES + row256, (chip * 2 + 1 - c) * LANES + row256 - LANES
    )

    @pl.loop(0, 64)
    def _(k):
        owned[:, columns_of(k)] = jnp.where(my_bus == ids_all[k], 1.0, 0.0).astype(jnp.bfloat16)

    hung = jnp.concatenate([my_ids[...], their_ids[...]], axis=1)
    down = lax.broadcasted_iota(jnp.int32, (LANES, 2 * LANES), 0)

    @pl.loop(0, 64)
    def _(k):
        buses = down + (k * 2 + c) * LANES
        chosen[columns_of(k), :] = jnp.where(hung == buses, 1.0, 0.0).astype(jnp.bfloat16)

    totals = gather_dot(blocks0, sems(1), owned, theirs.at[0], ours.at[0])
    bus_schur = totals[hours : hours + 1] + totals[hours + 1 : hours + 2]
    totals = totals[:hours]

    def flip(src, dst):
        @pl.loop(0, 64)
        def _(k):
            dst[columns_of(k), :] = src[:, columns_of(k)].T

    def bus_phase(totals, mu, step, bus_now, p):
        right = bus_load_ref[...] + mu * jax.nn.sigmoid(-bus_now) - totals
        pivots = diagonal_ref[...] + mu + bus_schur
        blocks[p, chip] = (right / pivots).astype(jnp.bfloat16)
        send(blocks.at[p], sems(p + 2))
        if p == 0:
            bytes_of(network.at[0:LANES], net_sems.at[0])
            bytes_of(network.at[LANES : 2 * LANES], net_sems.at[2])
            flip(owned, owned_turned)
        coupled = gather_dot(
            blocks.at[p],
            sems(p + 2),
            network_turned if p else network,
            theirs.at[p + 1],
            ours.at[p + 1],
            p > 0,
        )
        second = (right - coupled) / pivots
        blocks[p + 1, chip] = second.astype(jnp.bfloat16)
        send(blocks.at[p + 1], sems(p + 3))
        return bus_now + step * second

    bus_now = bus_phase(totals, mu, step_ref[0], bus_state_ref[...], 0)

    flip(network, network_turned)
    at = step_ref[0] * gather_dot(blocks.at[1], sems(3), chosen, theirs.at[2], ours.at[2], True)

    mu = barrier_ref[1]
    step = step_ref[0]

    def second_chunk(k, edge):
        start = pl.multiple_of(k * CHUNK, CHUNK)
        rows = response_ref[pl.ds(start, CHUNK), :]
        here = pltpu.roll(at, lax.rem(LANES - start, LANES), 1)
        for j in range(CHUNK):
            f = start + j
            row = rows[j : j + 1, :]
            now = state[f] + (step * solved[f] - row * here[:, j : j + 1])
            state[f] = now
            residual = (load[f].astype(jnp.float32) + mu * jax.nn.sigmoid(-now)).astype(jnp.bfloat16)
            load[f] = residual
            scaled = residual.astype(jnp.float32) * row
            term = jnp.sum(scaled[:, :LANES] + scaled[:, LANES:], axis=1, keepdims=True)
            edge = jnp.where(lane[:hours] == f, term, edge)
        return edge

    edge = lax.fori_loop(0, chunks, second_chunk, jnp.zeros((hours, LANES), jnp.float32))
    blocks[2, chip] = edge.astype(jnp.bfloat16)
    send(blocks.at[2], sems(4))
    last_step = step_ref[1]

    @pl.loop(0, chunks)
    def _(k):
        for j in range(CHUNK):
            f = k * CHUNK + j
            product = jnp.dot(load[f], inverse[f], preferred_element_type=jnp.float32)
            y_ref[f] = state[f] + last_step * product

    totals = gather_dot(blocks.at[2], sems(4), owned_turned, theirs.at[3], ours.at[3], True)
    bus_final_ref[...] = bus_phase(totals, mu, last_step, bus_now, 3)
    at_ref[...] = last_step * gather_dot(blocks.at[4], sems(6), chosen, theirs.at[5], ours.at[5], True)

    bytes_of(network.at[LANES : 2 * LANES], net_sems.at[1])
    others = pl.ds(0, len(OFFSETS))
    bytes_of(ids_all.at[others], sent.at[0])
    bytes_of(blocks0.at[others], sent.at[1])
    bytes_of(theirs.at[0], half_sent.at[1])
    for p in range(1, 6):
        bytes_of(theirs.at[p, 0:hours], half_sent.at[p + 1])
    for p in range(5):
        bytes_of(blocks.at[p, others], sent.at[p + 2])


def last_kernel(y_ref, response_ref, at_ref, bus_ref, out_hbm, bus_final_ref, out, sem):
    feeders = y_ref.shape[0]
    bus_final_ref[...] = bus_ref[...]

    def copy(k):
        rows = pl.ds(k * CHUNK, CHUNK)
        return pltpu.make_async_copy(out.at[rows], out_hbm.at[rows], sem.at[k])

    for k in range(feeders // CHUNK):
        for f in range(k * CHUNK, (k + 1) * CHUNK):
            out[f] = y_ref[f] - response_ref[f : f + 1, :] * at_ref[:, f : f + 1]
        copy(k).start()
    for k in range(feeders // CHUNK):
        copy(k).wait()


def on_device(
    feeder_state,
    feeder_load,
    feeder_inverse,
    coupling,
    feeder_bus,
    bus_coupling,
    bus_diagonal,
    bus_load,
    bus_state,
    barrier,
    step_length,
):
    feeders, hours, nodes = feeder_state.shape
    owned, buses = bus_coupling.shape
    f32, bf16 = jnp.float32, jnp.bfloat16
    vmem, smem = pl.BlockSpec(memory_space=pltpu.VMEM), pl.BlockSpec(memory_space=pltpu.SMEM)
    hbm = pl.BlockSpec(memory_space=pltpu.HBM)
    chunks = feeders // CHUNK
    y, response, at, bus_last = pl.pallas_call(
        kernel,
        name="interior_point",
        out_shape=[
            pltpu.VMEM((feeders, hours, nodes), f32),
            pltpu.VMEM((feeders, nodes), f32),
            pltpu.VMEM((hours, LANES), f32),
            pltpu.VMEM((hours, owned), f32),
        ],
        in_specs=[hbm, hbm, hbm, vmem, vmem, hbm, vmem, vmem, vmem, smem, smem],
        out_specs=[vmem, vmem, vmem, vmem],
        scratch_shapes=[
            pltpu.VMEM((feeders, nodes, nodes), bf16),
            pltpu.VMEM((feeders, hours, nodes), f32),
            pltpu.VMEM((feeders, hours, nodes), bf16),
            pltpu.VMEM((feeders, hours, nodes), f32),
            pltpu.VMEM((2 * owned, buses // 2), bf16),
            pltpu.VMEM((2 * owned, 64 * LANES), bf16),
            pltpu.VMEM((buses // 2, 2 * LANES), bf16),
            pltpu.VMEM((feeders, nodes), f32),
            pltpu.VMEM((64, hours + 8, LANES), bf16),
            pltpu.VMEM((5, 64, hours, LANES), bf16),
            pltpu.VMEM((64, 1, LANES), jnp.int32),
            pltpu.VMEM((1, LANES), jnp.int32),
            pltpu.VMEM((1, LANES), jnp.int32),
            pltpu.VMEM((6, hours + 8, LANES), f32),
            pltpu.VMEM((6, hours + 8, LANES), f32),
            pltpu.VMEM((64 * LANES, 2 * owned), bf16),
            pltpu.VMEM((buses // 2, 2 * owned), bf16),
            pltpu.SemaphoreType.DMA((3, chunks)),
            pltpu.SemaphoreType.DMA((3,)),
            pltpu.SemaphoreType.DMA((7,)),
            pltpu.SemaphoreType.DMA((7, 4)),
            pltpu.SemaphoreType.DMA((7,)),
            pltpu.SemaphoreType.DMA((7,)),
        ],
        compiler_params=pltpu.CompilerParams(
            collective_id=0, has_side_effects=True, vmem_limit_bytes=64_430_080
        ),
    )(
        feeder_state,
        feeder_load,
        feeder_inverse,
        coupling,
        feeder_bus.reshape(1, feeders),
        bus_coupling,
        bus_diagonal.reshape(1, owned),
        bus_load,
        bus_state,
        barrier,
        step_length,
    )
    return pl.pallas_call(
        last_kernel,
        name="last_update",
        out_shape=[
            jax.ShapeDtypeStruct((feeders, hours, nodes), f32),
            jax.ShapeDtypeStruct((hours, owned), f32),
        ],
        in_specs=[vmem, vmem, vmem, vmem],
        out_specs=[hbm, vmem],
        scratch_shapes=[
            pltpu.VMEM((feeders, hours, nodes), f32),
            pltpu.SemaphoreType.DMA((chunks,)),
        ],
        compiler_params=pltpu.CompilerParams(vmem_limit_bytes=8 * 2**20),
    )(y, response, at, bus_last)


def solution(mesh):
    in_specs = (
        P(BOTH, None, None),
        P(BOTH, None, None),
        P(BOTH, None, None),
        P(BOTH, None),
        P(BOTH),
        P(BOTH, None),
        P(BOTH),
        P(None, BOTH),
        P(None, BOTH),
        P(),
        P(),
    )
    out_specs = (P(BOTH, None, None), P(None, BOTH))
    return jax.shard_map(
        on_device, mesh=mesh, in_specs=in_specs, out_specs=out_specs, check_vma=False
    )
```
